32 devices in a mesh: shots: 2 (over y), rx: 4 (over z), ta: 2 (over x), af: 2 (over core).
Axes of the slice: x: 2, y: 2, z: 4, core: 2. Of those that a mesh axis runs over, the one named last changes fastest.
Arguments:
- traces: bfloat16 [4096, 512], P(('shots', 'rx'), ('ta', 'af')), parts along dimension 0, may hold values from -6 to 6
- slopes: int32 [512], replicated, may hold values from 0 to 1023
- offsets: int32 [4096], P('shots'), parts along dimension 0, may hold values from 1 to 4095
- live: int32 [4096], P('shots'), parts along dimension 0, may hold values 0 or 1
Outputs:
- stack: float32 [1024, 512], P(('shots', 'rx'), ('ta', 'af')), parts along dimension 0
- coherence: float32 [1024, 512], P(('shots', 'rx'), ('ta', 'af')), parts along dimension 0
- peak_values: float32 [1024], P(('shots', 'rx')), parts along dimension 0
The draws below stay inside these ranges and needn't reach their ends.
There are 2 independent parts, one for each index of `shots`. The reference program is written for one: setup_inputs(seed, part) draws one part's arguments, and reference() takes and returns one part's arrays. A program takes and returns all parts, laid end to end along the dimension named above; an argument that names none is the same for every part. Nothing has to cross between parts.
Inputs may be any that keep to these rules, and one draw needn't show every extreme that they name: delays are below 64: (slopes * offsets) // 65536 < 64.
All inputs are finite; a program needn't handle non-finite values.
Results may differ from the reference program's by a relative error of at most 0.0003.
Values may be sent and summed in bfloat16 or wider, within the bound.
A program may use at most 64 MiB of HBM per device.

```python
import jax
import jax.numpy as jnp
from jax import lax

RECV = 2048
SLOWS = 512
SPAN = 64
WIN = 16
NT = 512


def with_ends(values, rng, smallest, largest):
    index_at = [jax.random.randint(jax.random.fold_in(rng, axis), (), 0, length) for axis, length in enumerate(values.shape)]
    widest = values.shape.index(max(values.shape))
    neighbour = index_at[:widest] + [(index_at[widest] + 1) % values.shape[widest]] + index_at[widest + 1:]
    return values.at[tuple(index_at)].set(smallest).at[tuple(neighbour)].set(largest)


def steps_of(key, extent, cuts, smallest, high):
    factor_of = 1.0
    for position, shards_of in cuts:
        heights = jax.random.uniform(jax.random.fold_in(jax.random.fold_in(key, 6), position), (shards_of,), jnp.float32, smallest / len(cuts), high / len(cuts))
        factor_of = factor_of * jnp.repeat(jnp.exp(heights), extent[position] // shards_of).reshape((-1,) + (1,) * (len(extent) - 1 - position))
    return factor_of


def gaussian(key, extent, scale, limit, shards=(), held_as=jnp.bfloat16):
    result = scale * jax.random.normal(key, extent, jnp.float32)
    if shards:
        result = result * steps_of(key, extent, shards, -0.22, 0.18)
    return jnp.clip(result, -limit, limit).astype(held_as)


def setup_inputs(seed: int = 0, part: int = 0) -> dict:
    key_of = jax.random.split(jax.random.key(seed), 5)
    part_splits = jax.random.split(jax.random.fold_in(key_of[4], part), 5)
    traces = gaussian(part_splits[0], (RECV, NT), 1.0, 6.0, ((0, 4), (1, 4)))
    slopes = with_ends(jax.random.randint(key_of[1], (SLOWS,), 0, 16 * SPAN), jax.random.fold_in(key_of[1], 1), 0, (16 * SPAN) - 1).astype(jnp.int32)
    offsets = with_ends(jax.random.randint(part_splits[2], (RECV,), 1, 4096), jax.random.fold_in(part_splits[2], 1), 1, 4095).astype(jnp.int32)
    live = with_ends((jax.random.randint(part_splits[3], (RECV,), 0, 8) < 7).astype(jnp.int32), jax.random.fold_in(part_splits[3], 1), 0, 1)
    return dict(traces=traces, slopes=slopes, offsets=offsets, live=live)


def reference(traces, slopes, offsets, live):
    delays = (slopes[:, None] * offsets[None, :]) // 65536
    weighted = traces * live.astype(jnp.bfloat16)[:, None]
    squares = (weighted.astype(jnp.float32) ** 2).astype(jnp.bfloat16)
    padded_x = jnp.pad(weighted, ((0, 0), (0, SPAN)))
    padded_s = jnp.pad(squares, ((0, 0), (0, SPAN)))

    def lag_step(lag_index, carry):
        stack_acc, energy_acc = carry
        onehot = (delays == lag_index).astype(jnp.bfloat16)
        part_x = lax.dynamic_slice_in_dim(padded_x, lag_index, NT, 1)
        part_s = lax.dynamic_slice_in_dim(padded_s, lag_index, NT, 1)
        stack_acc = stack_acc + jnp.dot(onehot, part_x, preferred_element_type=jnp.float32)
        energy_acc = energy_acc + jnp.dot(onehot, part_s, preferred_element_type=jnp.float32)
        return stack_acc, energy_acc

    zeros = jnp.zeros((SLOWS, NT), jnp.float32)
    stack, energy = lax.fori_loop(0, SPAN, lag_step, (zeros, zeros))
    long_stack = jnp.pad(stack, ((0, 0), (0, WIN)))
    long_energy = jnp.pad(energy, ((0, 0), (0, WIN)))
    power_sum = jnp.zeros((SLOWS, NT), jnp.float32)
    energy_sum = jnp.zeros((SLOWS, NT), jnp.float32)
    for lag_index in range(WIN):
        power_sum = power_sum + long_stack[:, lag_index:lag_index + NT] ** 2
        energy_sum = energy_sum + long_energy[:, lag_index:lag_index + NT]
    coherence = power_sum / jnp.maximum(energy_sum, 1.0)
    peak_values = jnp.max(coherence, axis=1)
    return stack, coherence, peak_values
```

```python
import functools

import jax
import jax.numpy as jnp
from jax import lax
from jax.experimental import pallas as pl
from jax.experimental.pallas import tpu as pltpu
from jax.sharding import PartitionSpec as P

SPAN = 64
WIN = 16
PHASES = 16
MESH = pl.DeviceIdType.MESH
F32 = jnp.float32
BF16 = jnp.bfloat16


def window_sum(rows, width):
    reach = 1
    while reach < width:
        rows = rows[:-reach] + rows[reach:]
        reach *= 2
    return rows


def kernel(
    n_rx, n_ta, n_af, groups, halves,
    traces_ref, slopes_ref, offsets_ref, live_ref,
    stack_ref, coherence_ref, peak_ref,
    cols, halo, delays, long, parts, arrived, lead, lead_in, top, top_in,
    gather_send, gather_recv, halo_send, halo_recv,
    part_send, part_recv, lead_send, lead_recv, top_send, top_recv,
):
    blocks = n_ta * n_af
    members = n_rx // groups
    local_rows, block_len = traces_ref.shape
    half_rows = local_rows // halves
    group_slows = slopes_ref.shape[1] // groups
    own_slows = group_slows // members
    rx = lax.axis_index("rx")
    group, member = lax.div(rx, members), lax.rem(rx, members)
    other_rx = (groups - 1 - group) * members + member
    block = lax.axis_index("ta") * n_af + lax.axis_index("af")
    has_previous = block > 0
    has_next = block < blocks - 1

    def at_block(number):
        return {"ta": lax.div(number, n_af), "af": lax.rem(number, n_af)}

    previous = at_block(jnp.maximum(block - 1, 0))
    block_peers = [at_block(lax.rem(block + step, blocks)) for step in range(1, blocks)]
    member_peers = [lax.rem(member + step, members) for step in range(1, members)]

    peers = list(block_peers)
    peers += [{"rx": group * members + peer} for peer in member_peers]
    if groups > 1:
        peers.append({"rx": other_rx})
    barrier = pltpu.get_barrier_semaphore()
    for peer in peers:
        pl.semaphore_signal(barrier, inc=1, device_id=peer, device_id_type=MESH)

    for half in range(halves):
        rows = traces_ref[half * half_rows : (half + 1) * half_rows, :]
        cols[half] = rows.astype(F32).T.astype(BF16)

    @pl.when(jnp.logical_not(has_next))
    def _():
        halo[...] = jnp.zeros_like(halo)
        lead_in[...] = jnp.zeros_like(lead_in)

    pl.semaphore_wait(barrier, len(peers))

    def gather(half):
        return pltpu.make_async_remote_copy(
            src_ref=cols.at[half], dst_ref=cols.at[halves + half],
            send_sem=gather_send.at[half], recv_sem=gather_recv.at[half],
            device_id={"rx": other_rx}, device_id_type=MESH,
        )

    def pass_halo(index):
        return pltpu.make_async_remote_copy(
            src_ref=cols.at[index, pl.ds(0, SPAN)], dst_ref=halo.at[index],
            send_sem=halo_send.at[index], recv_sem=halo_recv.at[index],
            device_id=previous, device_id_type=MESH,
        )

    @pl.when(has_previous)
    def _():
        for half in range(halves):
            pass_halo(half).start()

    if groups > 1:
        for half in range(halves):
            gather(half).start()

    slopes = slopes_ref[:, pl.ds(pl.multiple_of(group * group_slows, group_slows), group_slows)]
    slopes = slopes.astype(F32)
    for index in range(groups * halves):
        side, half = divmod(index, halves)
        start = (other_rx if side else rx) * local_rows + half * half_rows
        lanes = pl.ds(pl.multiple_of(start, half_rows), half_rows)
        offsets = offsets_ref[:, lanes].astype(F32)
        marked = jnp.where(live_ref[:, lanes] != 0, offsets, 65536.0)
        column = jnp.broadcast_to(marked, (128, half_rows)).T
        column = jnp.concatenate([column] * (-(-group_slows // 128)), axis=1)[:, :group_slows]
        delay = jnp.floor(column * slopes * (1.0 / 65536.0))
        delays[index] = jnp.where(column < 65536.0, delay, 127.0).astype(BF16)

    parts[...] = jnp.zeros_like(parts)
    kept = block_len + SPAN - PHASES

    def add_block(index, carry):
        if groups > 1:
            @pl.when(jnp.logical_and(index >= 1, index <= halves))
            def _():
                gather(index - 1).wait_recv()

                @pl.when(has_previous)
                def _():
                    pass_halo(index - 1 + halves).start()

        @pl.when(has_next)
        def _():
            pass_halo(index).wait_recv()

        long[0:block_len] = cols[index].astype(F32)
        long[block_len:] = halo[index].astype(F32)
        delay = delays[index]
        for phase in range(PHASES):
            samples = long[phase : phase + kept]
            squares = (samples * samples).astype(BF16)
            samples = samples.astype(BF16)
            left, right = [], []
            for lag in range(0, SPAN, PHASES):
                left.append(jnp.concatenate(
                    [samples[lag : lag + block_len], squares[lag : lag + block_len]], axis=0))
                right.append(jnp.where(delay == jnp.asarray(lag + phase, BF16),
                                       jnp.asarray(1, BF16), jnp.asarray(0, BF16)))
            product = jnp.dot(jnp.concatenate(left, axis=1), jnp.concatenate(right, axis=0),
                              preferred_element_type=F32)
            for part in range(members):
                parts[part] += product[:, part * own_slows : (part + 1) * own_slows]
        return carry

    lax.fori_loop(0, groups * halves, add_block, 0)

    exchanges = []
    for step, peer in enumerate(member_peers):
        exchanges.append(pltpu.make_async_remote_copy(
            src_ref=parts.at[peer], dst_ref=arrived.at[step],
            send_sem=part_send.at[step], recv_sem=part_recv.at[step],
            device_id={"rx": group * members + peer}, device_id_type=MESH,
        ))
        exchanges[-1].start()
    total = parts[member]
    for step, exchange in enumerate(exchanges):
        exchange.wait_recv()
        total = total + arrived[step]

    stack, energy = total[:block_len], total[block_len:]
    lead[0:WIN] = stack[:WIN]
    lead[WIN:] = energy[:WIN]
    pass_lead = pltpu.make_async_remote_copy(
        src_ref=lead, dst_ref=lead_in, send_sem=lead_send, recv_sem=lead_recv,
        device_id=previous, device_id_type=MESH,
    )

    @pl.when(has_previous)
    def _():
        pass_lead.start()

    stack_ref[...] = stack.T

    @pl.when(has_next)
    def _():
        pass_lead.wait_recv()

    long_stack = jnp.concatenate([stack, lead_in[0:WIN]], axis=0)
    long_energy = jnp.concatenate([energy, lead_in[WIN:]], axis=0)
    power_sum = window_sum(long_stack * long_stack, WIN)[:block_len]
    energy_sum = window_sum(long_energy, WIN)[:block_len]
    coherence = power_sum / jnp.maximum(energy_sum, 1.0)
    peak = jnp.max(coherence, axis=0, keepdims=True)
    top[...] = peak
    tops = []
    for step, peer in enumerate(block_peers):
        tops.append(pltpu.make_async_remote_copy(
            src_ref=top, dst_ref=top_in.at[step],
            send_sem=top_send.at[step], recv_sem=top_recv.at[step],
            device_id=peer, device_id_type=MESH,
        ))
        tops[-1].start()
    coherence_ref[...] = coherence.T
    for step, copy in enumerate(tops):
        copy.wait_recv()
        peak = jnp.maximum(peak, top_in[step])
    peak_ref[...] = peak

    for copy in tops + exchanges:
        copy.wait_send()
    if groups > 1:
        for half in range(halves):
            gather(half).wait_send()

    @pl.when(has_previous)
    def _():
        pass_lead.wait_send()
        for index in range(groups * halves):
            pass_halo(index).wait_send()


def solution(mesh):
    n_rx, n_ta, n_af = (mesh.shape[name] for name in ("rx", "ta", "af"))
    groups = 2 if n_rx % 2 == 0 else 1
    members = n_rx // groups

    def on_device(traces, slopes, offsets, live):
        local_rows, block_len = traces.shape
        halves = 2 if local_rows % 512 == 0 else 1
        half_rows = local_rows // halves
        group_slows = slopes.shape[0] // groups
        own_slows = group_slows // members
        sides = groups * halves
        dma = pltpu.SemaphoreType.DMA
        blocks = n_ta * n_af
        vmem = pl.BlockSpec(memory_space=pltpu.VMEM)
        stack, coherence, peak = pl.pallas_call(
            functools.partial(kernel, n_rx, n_ta, n_af, groups, halves),
            out_shape=(
                jax.ShapeDtypeStruct((own_slows, block_len), F32),
                jax.ShapeDtypeStruct((own_slows, block_len), F32),
                jax.ShapeDtypeStruct((1, own_slows), F32),
            ),
            in_specs=[vmem] * 4,
            out_specs=(vmem,) * 3,
            scratch_shapes=[
                pltpu.VMEM((sides, block_len, half_rows), BF16),
                pltpu.VMEM((sides, SPAN, half_rows), BF16),
                pltpu.VMEM((sides, half_rows, group_slows), BF16),
                pltpu.VMEM((block_len + SPAN, half_rows), F32),
                pltpu.VMEM((members, 2 * block_len, own_slows), F32),
                pltpu.VMEM((max(members - 1, 1), 2 * block_len, own_slows), F32),
                pltpu.VMEM((2 * WIN, own_slows), F32),
                pltpu.VMEM((2 * WIN, own_slows), F32),
                pltpu.VMEM((1, own_slows), F32),
                pltpu.VMEM((max(blocks - 1, 1), 1, own_slows), F32),
                dma((halves,)), dma((halves,)),
                dma((sides,)), dma((sides,)),
                dma((max(members - 1, 1),)), dma((max(members - 1, 1),)),
                dma, dma,
                dma((max(blocks - 1, 1),)), dma((max(blocks - 1, 1),)),
            ],
            compiler_params=pltpu.CompilerParams(collective_id=0, has_side_effects=True),
            name="slant_stack",
        )(traces, slopes[None], offsets[None], live[None])
        return stack, coherence, peak[0]

    return jax.shard_map(
        on_device,
        mesh=mesh,
        in_specs=(P(("shots", "rx"), ("ta", "af")), P(), P("shots"), P("shots")),
        out_specs=(
            P(("shots", "rx"), ("ta", "af")),
            P(("shots", "rx"), ("ta", "af")),
            P(("shots", "rx")),
        ),
        check_vma=False,
    )
```

```python
import functools

import jax
import jax.numpy as jnp
from jax import lax
from jax.experimental import pallas as pl
from jax.experimental.pallas import tpu as pltpu
from jax.sharding import PartitionSpec as P

SPAN = 64
WIN = 16
PHASES = 16
MESH = pl.DeviceIdType.MESH
F32 = jnp.float32
BF16 = jnp.bfloat16


def window_sum(rows, width):
    reach = 1
    while reach < width:
        rows = rows[:-reach] + rows[reach:]
        reach *= 2
    return rows


def kernel(
    n_rx, n_ta, n_af, groups, halves,
    traces_ref, slopes_ref, offsets_ref, live_ref,
    stack_ref, coherence_ref, peak_ref,
    cols, halo, delays, long, parts, arrived, lead, lead_in, top, top_in,
    gather_send, gather_recv, halo_send, halo_recv,
    part_send, part_recv, lead_send, lead_recv, top_send, top_recv,
):
    blocks = n_ta * n_af
    members = n_rx // groups
    local_rows, block_len = traces_ref.shape
    half_rows = local_rows // halves
    group_slows = slopes_ref.shape[1] // groups
    own_slows = group_slows // members
    rx = lax.axis_index("rx")
    group, member = lax.div(rx, members), lax.rem(rx, members)
    other_rx = (groups - 1 - group) * members + member
    block = lax.axis_index("ta") * n_af + lax.axis_index("af")
    has_previous = block > 0
    has_next = block < blocks - 1

    def at_block(number):
        return {"ta": lax.div(number, n_af), "af": lax.rem(number, n_af)}

    previous = at_block(jnp.maximum(block - 1, 0))
    block_peers = [at_block(lax.rem(block + step, blocks)) for step in range(1, blocks)]
    member_peers = [lax.rem(member + step, members) for step in range(1, members)]

    peers = list(block_peers) + [{"rx": other_rx}]
    for peer in member_peers:
        peer_rx = {"rx": group * members + peer}
        peers.append(peer_rx)
        if blocks > 1:
            peers += [peer_rx | block_peers[0], peer_rx | block_peers[-1]]
    barrier = pltpu.get_barrier_semaphore()
    for peer in peers:
        pl.semaphore_signal(barrier, inc=1, device_id=peer, device_id_type=MESH)

    for half in range(halves):
        rows = traces_ref[half * half_rows : (half + 1) * half_rows, :]
        cols[half] = rows.astype(F32).T.astype(BF16)

    @pl.when(jnp.logical_not(has_next))
    def _():
        halo[...] = jnp.zeros_like(halo)
        lead_in[...] = jnp.zeros_like(lead_in)

    pl.semaphore_wait(barrier, len(peers))

    def gather(half):
        return pltpu.make_async_remote_copy(
            src_ref=cols.at[half], dst_ref=cols.at[halves + half],
            send_sem=gather_send.at[half], recv_sem=gather_recv.at[half],
            device_id={"rx": other_rx}, device_id_type=MESH,
        )

    def pass_halo(index):
        return pltpu.make_async_remote_copy(
            src_ref=cols.at[index, pl.ds(0, SPAN)], dst_ref=halo.at[index],
            send_sem=halo_send.at[index], recv_sem=halo_recv.at[index],
            device_id=previous, device_id_type=MESH,
        )

    @pl.when(has_previous)
    def _():
        for half in range(halves):
            pass_halo(half).start()

    for half in range(halves):
        gather(half).start()

    slopes = slopes_ref[:, pl.ds(pl.multiple_of(group * group_slows, group_slows), group_slows)]
    slopes = slopes.astype(F32)
    for index in range(groups * halves):
        side, half = divmod(index, halves)
        start = (other_rx if side else rx) * local_rows + half * half_rows
        lanes = pl.ds(pl.multiple_of(start, half_rows), half_rows)
        offsets = offsets_ref[:, lanes].astype(F32)
        marked = jnp.where(live_ref[:, lanes] != 0, offsets, 65536.0)
        column = jnp.broadcast_to(marked, (128, half_rows)).T
        column = jnp.concatenate([column] * (-(-group_slows // 128)), axis=1)[:, :group_slows]
        delay = jnp.floor(column * slopes * (1.0 / 65536.0))
        delays[index] = jnp.where(column < 65536.0, delay, 127.0).astype(BF16)

    parts[...] = jnp.zeros_like(parts)
    cut = block_len // 2
    kept = cut + SPAN - PHASES

    def add_block(index, upper):
        first = cut if upper else 0
        long[first:block_len] = cols[index, first:].astype(F32)
        if upper:
            long[block_len:] = halo[index].astype(F32)
        delay = delays[index]
        for phase in range(PHASES):
            samples = long[first + phase : first + phase + kept]
            squares = (samples * samples).astype(BF16)
            samples = samples.astype(BF16)
            left, right = [], []
            for lag in range(0, SPAN, PHASES):
                left.append(jnp.concatenate(
                    [samples[lag : lag + cut], squares[lag : lag + cut]], axis=0))
                right.append(jnp.where(delay == jnp.asarray(lag + phase, BF16),
                                       jnp.asarray(1, BF16), jnp.asarray(0, BF16)))
            product = jnp.dot(jnp.concatenate(left, axis=1), jnp.concatenate(right, axis=0),
                              preferred_element_type=F32)
            for part in range(members):
                parts[int(upper), part] += product[:, part * own_slows : (part + 1) * own_slows]

    def wait_halo(index):
        @pl.when(has_next)
        def _():
            pass_halo(index).wait_recv()

    def exchange(upper, step):
        peer = member_peers[step]
        return pltpu.make_async_remote_copy(
            src_ref=parts.at[upper, peer], dst_ref=arrived.at[upper, step],
            send_sem=part_send.at[upper, step], recv_sem=part_recv.at[upper, step],
            device_id={"rx": group * members + peer}, device_id_type=MESH,
        )

    def pass_lead(step):
        peer = lax.rem(member + step, members)
        return pltpu.make_async_remote_copy(
            src_ref=lead.at[peer], dst_ref=lead_in.at[step],
            send_sem=lead_send.at[step], recv_sem=lead_recv.at[step],
            device_id={"rx": group * members + peer} | previous, device_id_type=MESH,
        )

    def own_lower(half, carry):
        add_block(half, False)
        return carry

    def own_upper(half, carry):
        wait_halo(half)
        add_block(half, True)
        return carry

    def other_side(half, carry):
        gather(half).wait_recv()

        @pl.when(has_previous)
        def _():
            pass_halo(halves + half).start()

        add_block(halves + half, False)

        @pl.when(half == halves - 1)
        def _():
            for part in range(members):
                lead[part, 0:WIN] = parts[0, part, 0:WIN]
                lead[part, WIN:] = parts[0, part, cut : cut + WIN]

            @pl.when(has_previous)
            def _():
                for step in range(members):
                    pass_lead(step).start()

            for step in range(members - 1):
                exchange(0, step).start()

        wait_halo(halves + half)
        add_block(halves + half, True)
        return carry

    lax.fori_loop(0, halves, own_lower, 0)
    lax.fori_loop(0, halves, own_upper, 0)
    lax.fori_loop(0, halves, other_side, 0)
    for step in range(members - 1):
        exchange(1, step).start()

    totals = []
    for upper in range(2):
        total = parts[upper, member]
        for step in range(members - 1):
            exchange(upper, step).wait_recv()
            total = total + arrived[upper, step]
        stack_ref[:, upper * cut : (upper + 1) * cut] = total[:cut].T
        totals.append(total)
    stack = jnp.concatenate([total[:cut] for total in totals], axis=0)
    energy = jnp.concatenate([total[cut:] for total in totals], axis=0)

    @pl.when(has_next)
    def _():
        for step in range(members):
            pass_lead(step).wait_recv()

    following = lead_in[0]
    for step in range(1, members):
        following = following + lead_in[step]
    long_stack = jnp.concatenate([stack, following[:WIN]], axis=0)
    long_energy = jnp.concatenate([energy, following[WIN:]], axis=0)
    power_sum = window_sum(long_stack * long_stack, WIN)[:block_len]
    energy_sum = window_sum(long_energy, WIN)[:block_len]
    coherence = power_sum / jnp.maximum(energy_sum, 1.0)
    peak = jnp.max(coherence, axis=0, keepdims=True)
    top[...] = peak
    tops = []
    for step, peer in enumerate(block_peers):
        tops.append(pltpu.make_async_remote_copy(
            src_ref=top, dst_ref=top_in.at[step],
            send_sem=top_send.at[step], recv_sem=top_recv.at[step],
            device_id=peer, device_id_type=MESH,
        ))
        tops[-1].start()
    coherence_ref[...] = coherence.T
    for step, copy in enumerate(tops):
        copy.wait_recv()
        peak = jnp.maximum(peak, top_in[step])
    peak_ref[...] = peak

    for copy in tops:
        copy.wait_send()
    for step in range(members - 1):
        exchange(0, step).wait_send()
        exchange(1, step).wait_send()
    for half in range(halves):
        gather(half).wait_send()

    @pl.when(has_previous)
    def _():
        for step in range(members):
            pass_lead(step).wait_send()
        for index in range(groups * halves):
            pass_halo(index).wait_send()


def solution(mesh):
    n_rx, n_ta, n_af = (mesh.shape[name] for name in ("rx", "ta", "af"))
    groups = 2
    members = n_rx // groups

    def on_device(traces, slopes, offsets, live):
        local_rows, block_len = traces.shape
        halves = 2 if local_rows % 512 == 0 else 1
        half_rows = local_rows // halves
        group_slows = slopes.shape[0] // groups
        own_slows = group_slows // members
        sides = groups * halves
        dma = pltpu.SemaphoreType.DMA
        blocks = n_ta * n_af
        vmem = pl.BlockSpec(memory_space=pltpu.VMEM)
        stack, coherence, peak = pl.pallas_call(
            functools.partial(kernel, n_rx, n_ta, n_af, groups, halves),
            out_shape=(
                jax.ShapeDtypeStruct((own_slows, block_len), F32),
                jax.ShapeDtypeStruct((own_slows, block_len), F32),
                jax.ShapeDtypeStruct((1, own_slows), F32),
            ),
            in_specs=[vmem] * 4,
            out_specs=(vmem,) * 3,
            scratch_shapes=[
                pltpu.VMEM((sides, block_len, half_rows), BF16),
                pltpu.VMEM((sides, SPAN, half_rows), BF16),
                pltpu.VMEM((sides, half_rows, group_slows), BF16),
                pltpu.VMEM((block_len + SPAN, half_rows), F32),
                pltpu.VMEM((2, members, block_len, own_slows), F32),
                pltpu.VMEM((2, max(members - 1, 1), block_len, own_slows), F32),
                pltpu.VMEM((members, 2 * WIN, own_slows), F32),
                pltpu.VMEM((members, 2 * WIN, own_slows), F32),
                pltpu.VMEM((1, own_slows), F32),
                pltpu.VMEM((max(blocks - 1, 1), 1, own_slows), F32),
                dma((halves,)), dma((halves,)),
                dma((sides,)), dma((sides,)),
                dma((2, max(members - 1, 1))), dma((2, max(members - 1, 1))),
                dma((members,)), dma((members,)),
                dma((max(blocks - 1, 1),)), dma((max(blocks - 1, 1),)),
            ],
            compiler_params=pltpu.CompilerParams(collective_id=0, has_side_effects=True),
            name="slant_stack",
        )(traces, slopes[None], offsets[None], live[None])
        return stack, coherence, peak[0]

    return jax.shard_map(
        on_device,
        mesh=mesh,
        in_specs=(P(("shots", "rx"), ("ta", "af")), P(), P("shots"), P("shots")),
        out_specs=(
            P(("shots", "rx"), ("ta", "af")),
            P(("shots", "rx"), ("ta", "af")),
            P(("shots", "rx")),
        ),
        check_vma=False,
    )
```
